16 devices in a mesh: rep: 2 (over z), dp: 8 (over y, x, core).
Axes of the slice: x: 2, y: 2, z: 2, core: 2. Of those that a mesh axis runs over, the one named last changes fastest.
Arguments:
- hidden: bfloat16 [1024, 7168], P(('rep', 'dp')), parts along dimension 0
- ckv_cache: bfloat16 [1024, 256, 512], P(('rep', 'dp')), parts along dimension 0
- kpe_cache: bfloat16 [1024, 256, 64], P(('rep', 'dp')), parts along dimension 0
- cache_len: int32 [1024], P(('rep', 'dp')), parts along dimension 0
- rope_cos: float32 [1024, 32], P(('rep', 'dp')), parts along dimension 0
- rope_sin: float32 [1024, 32], P(('rep', 'dp')), parts along dimension 0
- norm_attn: float32 [7168], replicated
- w_dq: bfloat16 [7168, 1536], replicated
- norm_q: float32 [1536], replicated
- w_uq: bfloat16 [1536, 128, 192], replicated
- w_dkv: bfloat16 [7168, 576], replicated
- norm_kv: float32 [512], replicated
- w_uk: bfloat16 [512, 128, 128], replicated
- w_uv: bfloat16 [512, 128, 128], replicated
- w_out: bfloat16 [128, 128, 7168], replicated
- norm_mlp: float32 [7168], replicated
- w_gate: bfloat16 [7168, 18432], P(None, 'dp')
- w_up: bfloat16 [7168, 18432], P(None, 'dp')
- w_down: bfloat16 [18432, 7168], P('dp')
Outputs:
- output 1: bfloat16 [1024, 7168], P(('rep', 'dp')), parts along dimension 0
- output 2: bfloat16 [1024, 512], P(('rep', 'dp')), parts along dimension 0
- output 3: bfloat16 [1024, 64], P(('rep', 'dp')), parts along dimension 0
There are 2 independent parts. The reference program is written for one: setup_inputs(seed, part) draws one part's arguments, and reference() takes and returns one part's arrays. A program takes and returns all parts, laid end to end along the dimension named above; an argument that names none is the same for every part.
All inputs are finite; a program needn't handle non-finite values.
Results may differ from the reference program's by a relative error of at most 0.0109083.
Values are sent between devices in bfloat16 or wider.
A program may use at most 2 GiB of HBM per device.

```python
import math
import jax
import jax.numpy as jnp
from jax import lax

BATCH = 512
SEQ_LEN = 256
D_MODEL = 7168
HEADS = 128
Q_LORA = 1536
KV_LORA = 512
NOPE_DIM = 128
ROPE_DIM = 64
V_HEAD = 128
FF_DIM = 18432

EPSILON = 1e-6
MSCALE = 0.1 * math.log(40.0) + 1.0
SCORE_SCALE = MSCALE * MSCALE / math.sqrt(NOPE_DIM + ROPE_DIM)


def weight_draw(rand_key, arr_shape, fan_in):
    return (jax.random.normal(rand_key, arr_shape, jnp.float32) * fan_in ** -0.5).astype(jnp.bfloat16)


def gain_draw(rand_key, vec_size):
    return 1.0 + 0.3 * jax.random.normal(rand_key, (vec_size,), jnp.float32)


def setup_inputs(seed: int = 0, part: int = 0) -> dict:
    base_key = jax.random.key(seed)
    shared_keys = jax.random.split(base_key, 16)
    part_keys = jax.random.split(jax.random.fold_in(base_key, part), 8)
    half_rope = ROPE_DIM // 2
    hidden = jax.random.normal(part_keys[0], (BATCH, D_MODEL), jnp.float32).astype(jnp.bfloat16)
    centre = jax.random.normal(part_keys[1], (BATCH, 1, KV_LORA), jnp.float32)
    spread = jax.random.normal(part_keys[2], (BATCH, SEQ_LEN, KV_LORA), jnp.float32)
    ckv_cache = (0.6 * centre + 0.8 * spread).astype(jnp.bfloat16)
    kpe_cache = jax.random.normal(part_keys[3], (BATCH, SEQ_LEN, ROPE_DIM), jnp.float32).astype(jnp.bfloat16)
    base_len = jax.random.randint(part_keys[4], (BATCH,), 1, SEQ_LEN)
    pick_rows = jax.random.randint(part_keys[5], (2,), 0, BATCH)
    long_row = pick_rows[0]
    short_row = (long_row + 1 + pick_rows[1] % (BATCH - 1)) % BATCH
    cache_len = base_len.at[long_row].set(SEQ_LEN - 1).at[short_row].set(1)
    inv_freq = 10000.0 ** (-jnp.arange(half_rope, dtype=jnp.float32) / half_rope)
    angles = cache_len.astype(jnp.float32)[:, None] * inv_freq[None, :]
    return dict(
        hidden=hidden,
        ckv_cache=ckv_cache,
        kpe_cache=kpe_cache,
        cache_len=cache_len,
        rope_cos=jnp.cos(angles),
        rope_sin=jnp.sin(angles),
        norm_attn=gain_draw(shared_keys[0], D_MODEL),
        w_dq=weight_draw(shared_keys[1], (D_MODEL, Q_LORA), D_MODEL),
        norm_q=gain_draw(shared_keys[2], Q_LORA),
        w_uq=weight_draw(shared_keys[3], (Q_LORA, HEADS, NOPE_DIM + ROPE_DIM), Q_LORA),
        w_dkv=weight_draw(shared_keys[4], (D_MODEL, KV_LORA + ROPE_DIM), D_MODEL),
        norm_kv=gain_draw(shared_keys[5], KV_LORA),
        w_uk=weight_draw(shared_keys[6], (KV_LORA, HEADS, NOPE_DIM), NOPE_DIM),
        w_uv=weight_draw(shared_keys[7], (KV_LORA, HEADS, V_HEAD), KV_LORA),
        w_out=weight_draw(shared_keys[8], (HEADS, V_HEAD, D_MODEL), HEADS * V_HEAD),
        norm_mlp=gain_draw(shared_keys[9], D_MODEL),
        w_gate=weight_draw(shared_keys[10], (D_MODEL, FF_DIM), D_MODEL),
        w_up=weight_draw(shared_keys[11], (D_MODEL, FF_DIM), D_MODEL),
        w_down=weight_draw(shared_keys[12], (FF_DIM, D_MODEL), FF_DIM),
    )


def rms_norm(values_in, gain_vec):
    floats = values_in.astype(jnp.float32)
    mean_sq = jnp.mean(floats * floats, axis=-1, keepdims=True)
    return floats * lax.rsqrt(mean_sq + EPSILON) * gain_vec.astype(jnp.float32)


def apply_rope(values_in, cos_t, sin_t):
    half_dim = values_in.shape[-1] // 2
    low_half = values_in[..., :half_dim]
    high_half = values_in[..., half_dim:]
    return jnp.concatenate([low_half * cos_t - high_half * sin_t, high_half * cos_t + low_half * sin_t], axis=-1)


def one_request(operands):
    q_abs_row, q_pe_row, ckv_row, kpe_row, len_row, ckv_new_row, kpe_new_row = operands
    ckv_float = ckv_row.astype(jnp.float32)
    scores = (jnp.einsum('hl,tl->ht', q_abs_row.astype(jnp.float32), ckv_float)
              + jnp.einsum('hr,tr->ht', q_pe_row.astype(jnp.float32), kpe_row.astype(jnp.float32))) * SCORE_SCALE
    scores = jnp.where(jnp.arange(SEQ_LEN)[None, :] < len_row, scores, -jnp.inf)
    score_new = (jnp.dot(q_abs_row.astype(jnp.float32), ckv_new_row.astype(jnp.float32))
                 + jnp.dot(q_pe_row.astype(jnp.float32), kpe_new_row.astype(jnp.float32))) * SCORE_SCALE
    row_max = jnp.maximum(jnp.max(scores, axis=1), score_new)
    exp_cache = jnp.exp(scores - row_max[:, None])
    exp_new = jnp.exp(score_new - row_max)
    norm_sum = jnp.sum(exp_cache, axis=1) + exp_new
    weighted = (jnp.einsum('ht,tl->hl', exp_cache.astype(jnp.bfloat16).astype(jnp.float32), ckv_float)
                + exp_new.astype(jnp.bfloat16).astype(jnp.float32)[:, None] * ckv_new_row.astype(jnp.float32)[None, :])
    return (weighted / norm_sum[:, None]).astype(jnp.bfloat16)


def reference(hidden, ckv_cache, kpe_cache, cache_len, rope_cos, rope_sin, norm_attn, w_dq, norm_q, w_uq, w_dkv, norm_kv, w_uk, w_uv, w_out, norm_mlp, w_gate, w_up, w_down):
    normed = rms_norm(hidden, norm_attn).astype(jnp.bfloat16)
    q_latent = rms_norm(jnp.dot(normed, w_dq, preferred_element_type=jnp.float32), norm_q).astype(jnp.bfloat16)
    q_full = jnp.einsum('bl,lhe->bhe', q_latent.astype(jnp.float32), w_uq.astype(jnp.float32))
    q_nope = q_full[..., :NOPE_DIM].astype(jnp.bfloat16)
    q_pe = apply_rope(q_full[..., NOPE_DIM:], rope_cos[:, None, :], rope_sin[:, None, :]).astype(jnp.bfloat16)
    kv_full = jnp.dot(normed, w_dkv, preferred_element_type=jnp.float32)
    ckv_new = rms_norm(kv_full[:, :KV_LORA], norm_kv).astype(jnp.bfloat16)
    kpe_new = apply_rope(kv_full[:, KV_LORA:], rope_cos, rope_sin).astype(jnp.bfloat16)
    q_abs = jnp.einsum('bhn,lhn->bhl', q_nope.astype(jnp.float32), w_uk.astype(jnp.float32)).astype(jnp.bfloat16)
    lat_out = lax.map(one_request, (q_abs, q_pe, ckv_cache, kpe_cache, cache_len, ckv_new, kpe_new))
    head_out = jnp.einsum('bhl,lhv->bhv', lat_out.astype(jnp.float32), w_uv.astype(jnp.float32)).astype(jnp.bfloat16)
    attn_out = jnp.einsum('bhv,hvd->bd', head_out.astype(jnp.float32), w_out.astype(jnp.float32))
    residual = (hidden.astype(jnp.float32) + attn_out).astype(jnp.bfloat16)
    mlp_in = rms_norm(residual, norm_mlp).astype(jnp.bfloat16)
    gate_val = jnp.dot(mlp_in, w_gate, preferred_element_type=jnp.float32)
    up_val = jnp.dot(mlp_in, w_up, preferred_element_type=jnp.float32)
    act_val = (jax.nn.silu(gate_val) * up_val).astype(jnp.bfloat16)
    mlp_out = jnp.dot(act_val, w_down, preferred_element_type=jnp.float32)
    out_hidden = (residual.astype(jnp.float32) + mlp_out).astype(jnp.bfloat16)
    return (out_hidden, ckv_new, kpe_new)
```

```python
import functools
import math
import jax
import jax.numpy as jnp
from jax import lax
from jax.experimental import pallas as pl
from jax.experimental.pallas import tpu as pltpu
from jax.sharding import PartitionSpec as P

BF = jnp.bfloat16
F32 = jnp.float32
QS = 200
HS = 72
LC = 256


def start_rows(w_hbm, buf, sem, l0, count):
    def one(l, _):
        pltpu.make_async_copy(w_hbm.at[l0 + l], buf.at[:, pl.ds(pl.multiple_of(2 * l, 2), 2), :], sem).start()
        return 0
    lax.fori_loop(0, count, one, 0, unroll=8)


def spread(par):
    rows = lax.broadcasted_iota(jnp.int32, (128, 256), 0)
    cols = lax.broadcasted_iota(jnp.int32, (128, 256), 1)
    return jnp.where(cols == 2 * rows + par, 1.0, 0.0).astype(BF)


def uq_kernel(cq_ref, cos_ref, sin_ref, w_hbm, qn_ref, qr_ref, buf, acc, a2, q_scr, h_scr, sems):
    n_chunk = w_hbm.shape[0] // LC
    B = cq_ref.shape[0]
    P = w_hbm.shape[1]
    start_rows(w_hbm, buf.at[0], sems.at[0], 0, LC)
    for par in range(2):
        x = spread(par)
        for k in range(cq_ref.shape[1] // 128):
            a2[par * B:(par + 1) * B, k * 256:(k + 1) * 256] = jnp.dot(
                cq_ref[:, k * 128:(k + 1) * 128], x, preferred_element_type=F32).astype(BF)
    for c in range(n_chunk):
        slot = c % 2
        if c + 1 < n_chunk:
            start_rows(w_hbm, buf.at[1 - slot], sems.at[1 - slot], (c + 1) * LC, LC)
        pltpu.make_async_copy(buf.at[slot], buf.at[slot], sems.at[slot]).wait()
        lhs = a2[:, c * 2 * LC:(c + 1) * 2 * LC]

        def body(j, _):
            rhs = jnp.concatenate([buf[slot, 2 * j], buf[slot, 2 * j + 1]], axis=1)
            out = jnp.dot(lhs, rhs, preferred_element_type=F32)
            r0 = pl.multiple_of(j * 2 * B, 2 * B)
            if c > 0:
                out = out + acc[pl.ds(r0, 2 * B), :]
            if c < n_chunk - 1:
                acc[pl.ds(r0, 2 * B), :] = out
            else:
                for half in range(2):
                    for par in range(2):
                        q_scr[pl.ds(4 * j + 2 * half + par, B, stride=QS), :] = out[par * B:(par + 1) * B, half * 128:(half + 1) * 128]
            return 0
        lax.fori_loop(0, P // 2, body, 0, unroll=8)

    def tb(b, _):
        blk = q_scr[pl.ds(pl.multiple_of(b * QS, 8), 192), :]
        h_scr[pl.ds(b, 128, stride=HS), :] = blk[:128].T
        v = blk[128:192].T
        rot = jnp.concatenate([v[:, 32:], v[:, :32]], axis=1)
        qr_ref[b] = (v * cos_ref[pl.ds(b, 1), :] + rot * sin_ref[pl.ds(b, 1), :]).astype(BF)
        return 0
    lax.fori_loop(0, B, tb, 0, unroll=2)

    def hb(h, _):
        qn_ref[h] = h_scr[pl.ds(pl.multiple_of(h * HS, 8), B), :].astype(BF)
        return 0
    lax.fori_loop(0, 128, hb, 0, unroll=8)


def uq(cq, w_uq, cos2, sin2):
    B, L = cq.shape
    w4 = w_uq.transpose(0, 2, 1).reshape(L, 96, 2, 128)
    vm = pl.BlockSpec(memory_space=pltpu.VMEM)
    return pl.pallas_call(
        uq_kernel,
        in_specs=[vm, vm, vm, pl.BlockSpec(memory_space=pl.ANY)],
        out_specs=[vm, vm],
        out_shape=[jax.ShapeDtypeStruct((128, B, 128), BF), jax.ShapeDtypeStruct((B, 128, 64), BF)],
        scratch_shapes=[pltpu.VMEM((2, 96, 2 * LC, 128), BF), pltpu.VMEM((96 * B, 256), F32), pltpu.VMEM((2 * B, 2 * L), BF),
                        pltpu.VMEM((B * QS, 128), F32), pltpu.VMEM((128 * HS, 128), F32), pltpu.SemaphoreType.DMA((2,))],
        compiler_params=pltpu.CompilerParams(vmem_limit_bytes=60 * 1024 * 1024),
        cost_estimate=pl.CostEstimate(flops=2 * B * L * 24576, bytes_accessed=76 * 10**6, transcendentals=0),
        name="uq",
    )(cq, cos2, sin2, w4)


UL = 128
KS = 136


def uk_kernel(qn_ref, w_hbm, ql_ref, buf, scr, sel, sems):
    B = qn_ref.shape[1]
    n_chunk = w_hbm.shape[0] // UL
    P = w_hbm.shape[1]
    start_rows(w_hbm, buf.at[0], sems.at[0], 0, UL)
    sel[0:128] = spread(0)
    sel[128:256] = spread(1)
    for c in range(n_chunk):
        slot = c % 2
        if c + 1 < n_chunk:
            start_rows(w_hbm, buf.at[1 - slot], sems.at[1 - slot], (c + 1) * UL, UL)
        pltpu.make_async_copy(buf.at[slot], buf.at[slot], sems.at[slot]).wait()

        def body(j, _):
            rhs = jnp.concatenate([buf[slot, 2 * j], buf[slot, 2 * j + 1]], axis=1)
            w = jnp.dot(sel[...], rhs, preferred_element_type=F32).astype(BF)
            for half in range(2):
                for par in range(2):
                    h = 4 * j + 2 * half + par
                    out = lax.dot_general(qn_ref[h], w[par * UL:(par + 1) * UL, half * 128:(half + 1) * 128],
                                          (((1,), (1,)), ((), ())), preferred_element_type=F32)
                    scr[pl.ds(h, B, stride=KS), :] = out
            return 0
        lax.fori_loop(0, P // 2, body, 0, unroll=4)

        def cb(b, _):
            ql_ref[b, :, c * UL:(c + 1) * UL] = scr[pl.ds(pl.multiple_of(b * KS, 8), 128), :].astype(BF)
            return 0
        lax.fori_loop(0, B, cb, 0, unroll=4)


def uk(qn, w_uk):
    B = qn.shape[1]
    vm = pl.BlockSpec(memory_space=pltpu.VMEM)
    return pl.pallas_call(
        uk_kernel,
        in_specs=[vm, pl.BlockSpec(memory_space=pl.ANY)],
        out_specs=vm,
        out_shape=jax.ShapeDtypeStruct((B, 128, 512), BF),
        scratch_shapes=[pltpu.VMEM((2, 64, 2 * UL, 128), BF), pltpu.VMEM((B * KS, 128), F32), pltpu.VMEM((256, 256), BF),
                        pltpu.SemaphoreType.DMA((2,))],
        compiler_params=pltpu.CompilerParams(vmem_limit_bytes=60 * 1024 * 1024),
        cost_estimate=pl.CostEstimate(flops=2 * B * 128 * 128 * 512, bytes_accessed=26 * 10**6, transcendentals=0),
        name="uk",
    )(qn, w_uk.reshape(512, 64, 2, 128))


NB = 4


def attn_kernel(scale, len_ref, ql_ref, qr_ref, ckv_ref, kpe_ref, cn_ref, kn_ref, ol_ref):
    T = ckv_ref.shape[1]
    dn = (((1,), (1,)), ((), ()))
    for i in range(NB):
        pos = len_ref[pl.program_id(0) * NB + i]
        row = lax.broadcasted_iota(jnp.int32, ckv_ref.shape[1:], 0)
        ckv = jnp.where(row == pos, cn_ref[i], ckv_ref[i])
        lane = lax.broadcasted_iota(jnp.int32, (128, T), 1)
        kn = jnp.broadcast_to(kn_ref[i], (T, 64))
        s_new = lax.dot_general(qr_ref[i], kn, dn, preferred_element_type=F32)
        s_pe = jnp.dot(qr_ref[i], kpe_ref[i], preferred_element_type=F32)
        s = lax.dot_general(ql_ref[i], ckv, dn, preferred_element_type=F32)
        s = (s + jnp.where(lane == pos, s_new, s_pe)) * scale
        s = jnp.where(lane <= pos, s, -jnp.inf)
        e = jnp.exp(s - jnp.max(s, axis=1, keepdims=True))
        den = jnp.sum(e, axis=1, keepdims=True)
        ol = jnp.dot(e.astype(BF), ckv, preferred_element_type=F32)
        ol = (ol / den).astype(BF)
        for k in range(4):
            ol_ref[i, k] = ol[:, k * 128:(k + 1) * 128]


def attn(scale, length, ql, qr, ckv, kpe, c_new, k_new):
    B, T, L = ckv.shape
    spec = lambda *s: pl.BlockSpec((NB,) + s, lambda i, _: (i, 0, 0))
    return pl.pallas_call(
        functools.partial(attn_kernel, scale),
        grid_spec=pltpu.PrefetchScalarGridSpec(
            num_scalar_prefetch=1, grid=(B // NB,),
            in_specs=[spec(128, L), spec(128, 64), spec(T, L), spec(64, T), spec(1, L), spec(1, 64)],
            out_specs=pl.BlockSpec((NB, 4, 128, 128), lambda i, _: (i, 0, 0, 0))),
        out_shape=jax.ShapeDtypeStruct((B, 4, 128, 128), BF),
        compiler_params=pltpu.CompilerParams(vmem_limit_bytes=40 * 2**20),
        cost_estimate=pl.CostEstimate(flops=2 * B * 128 * T * 1100, bytes_accessed=40 * 10**6, transcendentals=B * 128 * T),
        name="attn",
    )(length, ql, qr, ckv, kpe.transpose(0, 2, 1), c_new.reshape(B, 1, L), k_new.reshape(B, 1, 64))


VP = 16


def uv_kernel(ol_hbm, w_hbm, o_ref, wbuf, abuf, sel, wsems, asem):
    B = ol_hbm.shape[0]
    n_chunk = 64 // VP

    def start_w(c, slot):
        def one(l, _):
            pltpu.make_async_copy(w_hbm.at[l, pl.ds(c * VP, VP)], wbuf.at[slot, :, pl.ds(pl.multiple_of(2 * l, 2), 2), :], wsems.at[slot]).start()
            return 0
        lax.fori_loop(0, 512, one, 0, unroll=8)
    def start_a(b, _):
        pltpu.make_async_copy(ol_hbm.at[b], abuf.at[:, :, pl.ds(pl.multiple_of(2 * b, 2), 2), :], asem).start()
        return 0
    lax.fori_loop(0, B, start_a, 0, unroll=8)
    start_w(0, 0)
    sel[0:128] = spread(0)
    sel[128:256] = spread(1)
    half_rows = lax.broadcasted_iota(jnp.int32, (2 * B, 2 * B), 0)
    half_cols = lax.broadcasted_iota(jnp.int32, (2 * B, 2 * B), 1)
    want = jnp.where(half_rows < B, 2 * half_rows, 2 * (half_rows - B) + 1)
    pick = jnp.where(half_cols == want, 1.0, 0.0).astype(BF)
    pltpu.make_async_copy(abuf, abuf, asem).wait()
    for c in range(n_chunk):
        slot = c % 2
        if c + 1 < n_chunk:
            start_w(c + 1, 1 - slot)
        pltpu.make_async_copy(wbuf.at[slot], wbuf.at[slot], wsems.at[slot]).wait()

        def body(j, _):
            p = c * VP + 2 * j
            out = [None, None]
            for k in range(4):
                rhs = jnp.concatenate([wbuf[slot, 2 * j, k * 256:(k + 1) * 256], wbuf[slot, 2 * j + 1, k * 256:(k + 1) * 256]], axis=1)
                w = jnp.dot(sel[...], rhs, preferred_element_type=F32).astype(BF)
                for half in range(2):
                    wh = w[:, half * 128:(half + 1) * 128]
                    wk = jnp.concatenate([wh[0:128], wh[128:256]], axis=1)
                    part = jnp.dot(abuf[k, p + half], wk, preferred_element_type=F32)
                    out[half] = part if out[half] is None else out[half] + part
            for half in range(2):
                r = jnp.dot(pick, out[half].astype(BF), preferred_element_type=F32).astype(BF)
                col = pl.multiple_of((p + half) * 256, 256)
                o_ref[:, pl.ds(col, 128)] = r[0:B, 0:128]
                o_ref[:, pl.ds(col + 128, 128)] = r[B:2 * B, 128:256]
            return 0
        lax.fori_loop(0, VP // 2, body, 0, unroll=2)


def uv(ol, w_uv):
    B = ol.shape[0]
    return pl.pallas_call(
        uv_kernel,
        in_specs=[pl.BlockSpec(memory_space=pl.ANY)] * 2,
        out_specs=pl.BlockSpec(memory_space=pltpu.VMEM),
        out_shape=jax.ShapeDtypeStruct((B, 128 * 128), BF),
        scratch_shapes=[pltpu.VMEM((2, VP, 1024, 128), BF), pltpu.VMEM((4, 64, 2 * B, 128), BF), pltpu.VMEM((256, 256), BF),
                        pltpu.SemaphoreType.DMA((2,)), pltpu.SemaphoreType.DMA],
        compiler_params=pltpu.CompilerParams(vmem_limit_bytes=60 * 1024 * 1024),
        cost_estimate=pl.CostEstimate(flops=2 * B * 128 * 128 * 512, bytes_accessed=26 * 10**6, transcendentals=0),
        name="uv",
    )(ol.reshape(B, 4, 64, 2, 128), w_uv.reshape(512, 64, 2, 128))

EPSILON = 1e-6
MSCALE = 0.1 * math.log(40.0) + 1.0


def rms_norm(values_in, gain_vec):
    floats = values_in.astype(jnp.float32)
    mean_sq = jnp.mean(floats * floats, axis=-1, keepdims=True)
    return floats * lax.rsqrt(mean_sq + EPSILON) * gain_vec


def apply_rope(values_in, cos_t, sin_t):
    half_dim = values_in.shape[-1] // 2
    low_half = values_in[..., :half_dim]
    high_half = values_in[..., half_dim:]
    return jnp.concatenate([low_half * cos_t - high_half * sin_t, high_half * cos_t + low_half * sin_t], axis=-1)


def attention_rows(hidden, ckv_cache, kpe_cache, cache_len, rope_cos, rope_sin, norm_attn, w_dq, norm_q, w_uq, w_dkv, norm_kv, w_uk, w_uv, w_out):
    value_dim = w_uk.shape[0]
    score_scale = MSCALE * MSCALE / math.sqrt(w_uq.shape[2])
    normed = rms_norm(hidden, norm_attn).astype(BF)
    q_latent = rms_norm(jnp.dot(normed, w_dq, preferred_element_type=jnp.float32), norm_q).astype(BF)
    kv_full = jnp.dot(normed, w_dkv, preferred_element_type=jnp.float32)
    ckv_new = rms_norm(kv_full[:, :value_dim], norm_kv).astype(BF)
    kpe_new = apply_rope(kv_full[:, value_dim:], rope_cos, rope_sin).astype(BF)
    qn, qr = uq(q_latent, w_uq, jnp.concatenate([rope_cos, rope_cos], axis=1), jnp.concatenate([-rope_sin, rope_sin], axis=1))
    ql = uk(qn, w_uk)
    ol = attn(score_scale, cache_len, ql, qr, ckv_cache, kpe_cache, ckv_new, kpe_new)
    head_out = uv(ol, w_uv)
    attn_out = jnp.dot(head_out, w_out.reshape(-1, w_out.shape[2]), preferred_element_type=jnp.float32)
    residual = (hidden.astype(jnp.float32) + attn_out).astype(BF)
    return residual, ckv_new, kpe_new


def solution(mesh):
    row_spec = P(('rep', 'dp'), None)
    cube_spec = P(('rep', 'dp'), None, None)
    full_spec = P()
    in_specs = (row_spec, cube_spec, cube_spec, P(('rep', 'dp')), row_spec, row_spec,
                full_spec, full_spec, full_spec, full_spec, full_spec, full_spec, full_spec, full_spec, full_spec, full_spec,
                P(None, 'dp'), P(None, 'dp'), P('dp', None))

    def local_step(hidden, ckv_cache, kpe_cache, cache_len, rope_cos, rope_sin, norm_attn, w_dq, norm_q, w_uq, w_dkv, norm_kv, w_uk, w_uv, w_out, norm_mlp, w_gate, w_up, w_down):
        residual, ckv_new, kpe_new = attention_rows(hidden, ckv_cache, kpe_cache, cache_len, rope_cos, rope_sin, norm_attn, w_dq, norm_q, w_uq, w_dkv, norm_kv, w_uk, w_uv, w_out)
        mlp_in = rms_norm(residual, norm_mlp).astype(jnp.bfloat16)
        group_in = lax.all_gather(mlp_in, 'dp', axis=0, tiled=True)
        gate_val = jnp.dot(group_in, w_gate, preferred_element_type=jnp.float32)
        up_val = jnp.dot(group_in, w_up, preferred_element_type=jnp.float32)
        act_val = (jax.nn.silu(gate_val) * up_val).astype(jnp.bfloat16)
        partial_sum = jnp.dot(act_val, w_down, preferred_element_type=jnp.float32)
        mlp_rows = lax.psum_scatter(partial_sum, 'dp', scatter_dimension=0, tiled=True)
        out_hidden = (residual.astype(jnp.float32) + mlp_rows).astype(jnp.bfloat16)
        return out_hidden, ckv_new, kpe_new

    return jax.shard_map(local_step, mesh=mesh, in_specs=in_specs, out_specs=(row_spec, row_spec, row_spec), check_vma=False)
```

```python
import functools
import math
import jax
import jax.numpy as jnp
from jax import lax
from jax.experimental import pallas as pl
from jax.experimental.pallas import tpu as pltpu
from jax.sharding import PartitionSpec as P

EPSILON = 1e-6
MSCALE = 0.1 * math.log(40.0) + 1.0
BF = jnp.bfloat16
F32 = jnp.float32
LANES = 128
WIDE = 256
LATENT = 512
NT = (((1,), (1,)), ((), ()))
VMEM_BYTES = 60 * 1024 * 1024
QS = 200
HS = 72
LC = 256


def start_rows(w_hbm, buf, sem, l0, count):
    def one(l, _):
        pltpu.make_async_copy(w_hbm.at[l0 + l], buf.at[:, pl.ds(pl.multiple_of(2 * l, 2), 2), :], sem).start()
        return 0
    lax.fori_loop(0, count, one, 0, unroll=8)


def spread(par):
    rows = lax.broadcasted_iota(jnp.int32, (LANES, WIDE), 0)
    cols = lax.broadcasted_iota(jnp.int32, (LANES, WIDE), 1)
    return jnp.where(cols == 2 * rows + par, 1.0, 0.0).astype(BF)


def uq_kernel(cq_ref, cos_ref, sin_ref, w_hbm, qn_ref, qr_ref, buf, acc, a2, q_scr, h_scr, sems):
    n_chunk = w_hbm.shape[0] // LC
    B = cq_ref.shape[0]
    P = w_hbm.shape[1]
    start_rows(w_hbm, buf.at[0], sems.at[0], 0, LC)
    for par in range(2):
        x = spread(par)
        for k in range(cq_ref.shape[1] // LANES):
            a2[par * B:(par + 1) * B, k * WIDE:(k + 1) * WIDE] = jnp.dot(
                cq_ref[:, k * LANES:(k + 1) * LANES], x, preferred_element_type=F32).astype(BF)
    for c in range(n_chunk):
        slot = c % 2
        if c + 1 < n_chunk:
            start_rows(w_hbm, buf.at[1 - slot], sems.at[1 - slot], (c + 1) * LC, LC)
        pltpu.make_async_copy(buf.at[slot], buf.at[slot], sems.at[slot]).wait()
        lhs = a2[:, c * 2 * LC:(c + 1) * 2 * LC]

        def body(j, _):
            rhs = jnp.concatenate([buf[slot, 2 * j], buf[slot, 2 * j + 1]], axis=1)
            out = jnp.dot(lhs, rhs, preferred_element_type=F32)
            r0 = pl.multiple_of(j * 2 * B, 2 * B)
            if c > 0:
                out = out + acc[pl.ds(r0, 2 * B), :]
            if c < n_chunk - 1:
                acc[pl.ds(r0, 2 * B), :] = out
            else:
                for half in range(2):
                    for par in range(2):
                        q_scr[pl.ds(4 * j + 2 * half + par, B, stride=QS), :] = out[par * B:(par + 1) * B, half * LANES:(half + 1) * LANES]
            return 0
        lax.fori_loop(0, P // 2, body, 0, unroll=8)

    def tb(b, _):
        blk = q_scr[pl.ds(pl.multiple_of(b * QS, 8), 192), :]
        h_scr[pl.ds(b, LANES, stride=HS), :] = blk[:LANES].T
        v = blk[LANES:192].T
        rot = jnp.concatenate([v[:, 32:], v[:, :32]], axis=1)
        qr_ref[b] = (v * cos_ref[pl.ds(b, 1), :] + rot * sin_ref[pl.ds(b, 1), :]).astype(BF)
        return 0
    lax.fori_loop(0, B, tb, 0, unroll=8)

    def hb(h, _):
        qn_ref[h] = h_scr[pl.ds(pl.multiple_of(h * HS, 8), B), :].astype(BF)
        return 0
    lax.fori_loop(0, LANES, hb, 0, unroll=8)


def uq(cq, w_uq, cos2, sin2):
    B, L = cq.shape
    w4 = w_uq.transpose(0, 2, 1).reshape(L, 96, 2, LANES)
    vm = pl.BlockSpec(memory_space=pltpu.VMEM)
    return pl.pallas_call(
        uq_kernel,
        in_specs=[vm, vm, vm, pl.BlockSpec(memory_space=pl.ANY)],
        out_specs=[vm, vm],
        out_shape=[jax.ShapeDtypeStruct((LANES, B, LANES), BF), jax.ShapeDtypeStruct((B, LANES, 64), BF)],
        scratch_shapes=[pltpu.VMEM((2, 96, 2 * LC, LANES), BF), pltpu.VMEM((96 * B, WIDE), F32), pltpu.VMEM((2 * B, 2 * L), BF),
                        pltpu.VMEM((B * QS, LANES), F32), pltpu.VMEM((LANES * HS, LANES), F32), pltpu.SemaphoreType.DMA((2,))],
        compiler_params=pltpu.CompilerParams(vmem_limit_bytes=VMEM_BYTES),
        cost_estimate=pl.CostEstimate(flops=2 * B * L * 24576, bytes_accessed=76 * 10**6, transcendentals=0),
        name="uq",
    )(cq, cos2, sin2, w4)


UL = LANES
KS = 136


def uk_kernel(qn_ref, w_hbm, ql_ref, buf, scr, wd, sel, sems):
    B = qn_ref.shape[1]
    n_chunk = w_hbm.shape[0] // UL
    P = w_hbm.shape[1]
    start_rows(w_hbm, buf.at[0], sems.at[0], 0, UL)
    sel[0:LANES] = spread(0)
    sel[LANES:WIDE] = spread(1)
    for c in range(n_chunk):
        slot = c % 2
        if c + 1 < n_chunk:
            start_rows(w_hbm, buf.at[1 - slot], sems.at[1 - slot], (c + 1) * UL, UL)
        pltpu.make_async_copy(buf.at[slot], buf.at[slot], sems.at[slot]).wait()

        def sort(j, _):
            rhs = jnp.concatenate([buf[slot, 2 * j], buf[slot, 2 * j + 1]], axis=1)
            wd[j] = jnp.dot(sel[...], rhs, preferred_element_type=F32).astype(BF)
            return 0
        lax.fori_loop(0, P // 2, sort, 0, unroll=8)

        def body(j, _):
            for half in range(2):
                for par in range(2):
                    h = 4 * j + 2 * half + par
                    scr[pl.ds(h, B, stride=KS), :] = lax.dot_general(
                        qn_ref[h], wd[j, par * UL:(par + 1) * UL, half * LANES:(half + 1) * LANES],
                        NT, preferred_element_type=F32)
            return 0
        lax.fori_loop(0, P // 2, body, 0, unroll=4)

        def cb(b, _):
            ql_ref[b, :, c * UL:(c + 1) * UL] = scr[pl.ds(pl.multiple_of(b * KS, 8), LANES), :].astype(BF)
            return 0
        lax.fori_loop(0, B, cb, 0, unroll=4)


def uk(qn, w_uk):
    B = qn.shape[1]
    vm = pl.BlockSpec(memory_space=pltpu.VMEM)
    return pl.pallas_call(
        uk_kernel,
        in_specs=[vm, pl.BlockSpec(memory_space=pl.ANY)],
        out_specs=vm,
        out_shape=jax.ShapeDtypeStruct((B, LANES, LATENT), BF),
        scratch_shapes=[pltpu.VMEM((2, 64, 2 * UL, LANES), BF), pltpu.VMEM((B * KS, LANES), F32), pltpu.VMEM((32, WIDE, WIDE), BF), pltpu.VMEM((WIDE, WIDE), BF),
                        pltpu.SemaphoreType.DMA((2,))],
        compiler_params=pltpu.CompilerParams(vmem_limit_bytes=VMEM_BYTES),
        cost_estimate=pl.CostEstimate(flops=2 * B * LANES * LANES * LATENT, bytes_accessed=26 * 10**6, transcendentals=0),
        name="uk",
    )(qn, w_uk.reshape(LATENT, 64, 2, LANES))


NB = 4


def attn_kernel(scale, len_ref, ql_ref, qr_ref, ckv_ref, kpe_ref, cn_ref, kn_ref, ol_ref):
    T = ckv_ref.shape[1]
    dn = NT
    for i in range(NB):
        pos = len_ref[pl.program_id(0) * NB + i]
        row = lax.broadcasted_iota(jnp.int32, ckv_ref.shape[1:], 0)
        ckv = jnp.where(row == pos, cn_ref[i], ckv_ref[i])
        lane = lax.broadcasted_iota(jnp.int32, (LANES, T), 1)
        kn = jnp.broadcast_to(kn_ref[i], (T, 64))
        s_new = lax.dot_general(qr_ref[i], kn, dn, preferred_element_type=F32)
        s_pe = jnp.dot(qr_ref[i], kpe_ref[i], preferred_element_type=F32)
        s = lax.dot_general(ql_ref[i], ckv, dn, preferred_element_type=F32)
        s = (s + jnp.where(lane == pos, s_new, s_pe)) * scale
        s = jnp.where(lane <= pos, s, -jnp.inf)
        e = jnp.exp(s - jnp.max(s, axis=1, keepdims=True))
        den = jnp.sum(e, axis=1, keepdims=True)
        ol = jnp.dot(e.astype(BF), ckv, preferred_element_type=F32)
        ol = (ol / den).astype(BF)
        for k in range(4):
            ol_ref[i, k] = ol[:, k * LANES:(k + 1) * LANES]


def attn(scale, length, ql, qr, ckv, kpe, c_new, k_new):
    B, T, L = ckv.shape
    spec = lambda *s: pl.BlockSpec((NB,) + s, lambda i, _: (i, 0, 0))
    return pl.pallas_call(
        functools.partial(attn_kernel, scale),
        grid_spec=pltpu.PrefetchScalarGridSpec(
            num_scalar_prefetch=1, grid=(B // NB,),
            in_specs=[spec(LANES, L), spec(LANES, 64), spec(T, L), spec(64, T), spec(1, L), spec(1, 64)],
            out_specs=pl.BlockSpec((NB, 4, LANES, LANES), lambda i, _: (i, 0, 0, 0))),
        out_shape=jax.ShapeDtypeStruct((B, 4, LANES, LANES), BF),
        compiler_params=pltpu.CompilerParams(vmem_limit_bytes=40 * 2**20),
        cost_estimate=pl.CostEstimate(flops=2 * B * LANES * T * 1100, bytes_accessed=40 * 10**6, transcendentals=B * LANES * T),
        name="attn",
    )(length, ql, qr, ckv, kpe.transpose(0, 2, 1), c_new.reshape(B, 1, L), k_new.reshape(B, 1, 64))


VP = 16


def uv_kernel(ol_hbm, w_hbm, o_ref, wbuf, abuf, wd, mid, sel, wsems, asem):
    B = ol_hbm.shape[0]
    n_chunk = 64 // VP

    def start_w(c, slot):
        def one(l, _):
            pltpu.make_async_copy(w_hbm.at[l, pl.ds(c * VP, VP)], wbuf.at[slot, :, pl.ds(pl.multiple_of(2 * l, 2), 2), :], wsems.at[slot]).start()
            return 0
        lax.fori_loop(0, LATENT, one, 0, unroll=8)
    def start_a(b, _):
        pltpu.make_async_copy(ol_hbm.at[b], abuf.at[:, :, pl.ds(pl.multiple_of(2 * b, 2), 2), :], asem).start()
        return 0
    lax.fori_loop(0, B, start_a, 0, unroll=8)
    start_w(0, 0)
    sel[0:LANES] = spread(0)
    sel[LANES:WIDE] = spread(1)
    half_rows = lax.broadcasted_iota(jnp.int32, (2 * B, 2 * B), 0)
    half_cols = lax.broadcasted_iota(jnp.int32, (2 * B, 2 * B), 1)
    want = jnp.where(half_rows < B, 2 * half_rows, 2 * (half_rows - B) + 1)
    pick = jnp.where(half_cols == want, 1.0, 0.0).astype(BF)
    pltpu.make_async_copy(abuf, abuf, asem).wait()
    for c in range(n_chunk):
        slot = c % 2
        if c + 1 < n_chunk:
            start_w(c + 1, 1 - slot)
        pltpu.make_async_copy(wbuf.at[slot], wbuf.at[slot], wsems.at[slot]).wait()

        def sort(j, _):
            for k in range(4):
                rows = slice(k * WIDE, (k + 1) * WIDE)
                rhs = jnp.concatenate([wbuf[slot, 2 * j, rows], wbuf[slot, 2 * j + 1, rows]], axis=1)
                w = jnp.dot(sel[...], rhs, preferred_element_type=F32).astype(BF)
                for half in range(2):
                    for par in range(2):
                        wd[2 * j + half, k * LANES:(k + 1) * LANES, par * LANES:(par + 1) * LANES] = w[par * LANES:(par + 1) * LANES, half * LANES:(half + 1) * LANES]
            return 0
        lax.fori_loop(0, VP // 2, sort, 0, unroll=2)

        def body(j, _):
            p = c * VP + j
            lhs = jnp.concatenate([abuf[k, p] for k in range(4)], axis=1)
            mid[j] = jnp.dot(lhs, wd[j], preferred_element_type=F32).astype(BF)
            return 0
        lax.fori_loop(0, VP, body, 0, unroll=4)

        def put(j, _):
            r = jnp.dot(pick, mid[j], preferred_element_type=F32).astype(BF)
            col = pl.multiple_of((c * VP + j) * WIDE, WIDE)
            o_ref[:, pl.ds(col, LANES)] = r[0:B, 0:LANES]
            o_ref[:, pl.ds(col + LANES, LANES)] = r[B:2 * B, LANES:WIDE]
            return 0
        lax.fori_loop(0, VP, put, 0, unroll=4)


def uv(ol, w_uv):
    B = ol.shape[0]
    return pl.pallas_call(
        uv_kernel,
        in_specs=[pl.BlockSpec(memory_space=pl.ANY)] * 2,
        out_specs=pl.BlockSpec(memory_space=pltpu.VMEM),
        out_shape=jax.ShapeDtypeStruct((B, LANES * LANES), BF),
        scratch_shapes=[pltpu.VMEM((2, VP, 1024, LANES), BF), pltpu.VMEM((4, 64, 2 * B, LANES), BF), pltpu.VMEM((VP, LATENT, WIDE), BF), pltpu.VMEM((VP, 2 * B, WIDE), BF), pltpu.VMEM((WIDE, WIDE), BF),
                        pltpu.SemaphoreType.DMA((2,)), pltpu.SemaphoreType.DMA],
        compiler_params=pltpu.CompilerParams(vmem_limit_bytes=VMEM_BYTES),
        cost_estimate=pl.CostEstimate(flops=2 * B * LANES * LANES * LATENT, bytes_accessed=26 * 10**6, transcendentals=0),
        name="uv",
    )(ol.reshape(B, 4, 64, 2, LANES), w_uv.reshape(LATENT, 64, 2, LANES))

def here():
    d = lax.axis_index("dp")
    core = lax.rem(d, 2)
    x = lax.rem(d // 2, 2)
    y = d // 4
    partner = {"dp": d + 1 - 2 * core}
    xn = {"dp": d + 2 - 4 * x}
    yn = {"dp": d + 4 - 8 * y}
    chips = dict(me=2 * y + x, xn=2 * y + 1 - x, yn=2 * (1 - y) + x, diag=2 * (1 - y) + 1 - x)
    return core, chips, partner, xn, yn


def greet(devices):
    barrier = pltpu.get_barrier_semaphore()
    for dev in devices:
        pl.semaphore_signal(barrier, inc=1, device_id=dev, device_id_type=pl.DeviceIdType.MESH)
    pl.semaphore_wait(barrier, len(devices))


def remote(src, dst, send_sem, recv_sem, dev):
    return pltpu.make_async_remote_copy(src_ref=src, dst_ref=dst, send_sem=send_sem, recv_sem=recv_sem,
                                        device_id=dev, device_id_type=pl.DeviceIdType.MESH)


RT = WIDE


def out_kernel(o_ref, x_ref, g_ref, w_hbm, u_ref, r_ref, o2, x2, rall, wbuf, wsems, osems, ssems, rsems):
    core, chips, partner, xn, yn = here()
    me = chips["me"]
    D = x_ref.shape[1]
    half = D // 2
    K = o_ref.shape[1]
    B = o_ref.shape[0]
    n_tile = half // RT
    mine = pl.ds(pl.multiple_of(core * B, B), B)

    def cols(t):
        return pl.ds(pl.multiple_of(core * half + t * RT, RT), RT)

    def load_w(t, slot):
        return pltpu.make_async_copy(w_hbm.at[:, cols(t)], wbuf.at[slot], wsems.at[slot])
    load_w(0, 0).start()
    load_w(1, 1).start()
    greet((partner, xn, yn))
    send_o = remote(o_ref, o2.at[mine], osems.at[0], osems.at[1], partner)
    send_o.start()
    theirs = pl.ds(pl.multiple_of((1 - core) * half, half), half)
    send_x = remote(x_ref.at[:, theirs], x2.at[mine], osems.at[2], osems.at[3], partner)
    send_x.start()
    o2[mine, :] = o_ref[...]
    x2[mine, :] = x_ref[:, pl.ds(pl.multiple_of(core * half, half), half)]

    def copy(flow, t, chip, dev):
        ref = rall.at[chips[chip], :, cols(t)]
        return remote(ref, ref, ssems.at[flow, t], rsems.at[flow, t], dev)

    def arrival(flow, t, chip):
        ref = rall.at[chips[chip], :, cols(t)]
        return remote(ref, ref, ssems.at[flow, t], rsems.at[flow, t], partner)

    def first_forwards(t, par):
        arrival(1, t, "xn").wait_recv()
        copy(3, t, "xn", partner).start()
        if par == 0:
            copy(4, t, "xn", yn).start()
        arrival(2, t, "yn").wait_recv()
        copy(5, t, "yn", partner).start()
        if par == 1:
            copy(4, t, "yn", xn).start()

    def last_forward(t):
        arrival(4, t, "diag").wait_recv()
        copy(6, t, "diag", partner).start()
    send_o.wait()
    send_x.wait()

    def pair(i, _):
        for par in range(2):
            t = 2 * i + par
            load_w(t, par).wait()
            def dot_k(k, acc):
                rows = pl.ds(pl.multiple_of(k * 2048, 2048), 2048)
                return acc + jnp.dot(o2[:, rows], wbuf[par, rows, :], preferred_element_type=F32)
            acc = lax.fori_loop(0, K // 2048, dot_k, jnp.zeros((2 * B, RT), F32), unroll=4)
            xt = x2[:, pl.ds(pl.multiple_of(t * RT, RT), RT)].astype(F32)
            rall[me, :, cols(t)] = (xt + acc).astype(BF)

            @pl.when(i < n_tile // 2 - 1)
            def _():
                load_w(t + 2, par).start()
            copy(0, t, "me", partner).start()
            copy(1, t, "me", xn).start()
            copy(2, t, "me", yn).start()

            @pl.when(i > 0)
            def _():
                first_forwards(t - 2, par)

            @pl.when(i > 1)
            def _():
                last_forward(t - 4)
        return 0
    lax.fori_loop(0, n_tile // 2, pair, 0)
    for par in range(2):
        first_forwards(n_tile - 2 + par, par)
    for t in range(n_tile - 4, n_tile):
        last_forward(t)

    def finish(t, _):
        other = pl.ds(pl.multiple_of((1 - core) * half + t * RT, RT), RT)
        for flow, chip in ((0, "me"), (3, "xn"), (5, "yn"), (6, "diag")):
            ref = rall.at[chips[chip], :, other]
            remote(ref, ref, ssems.at[flow, t], rsems.at[flow, t], partner).wait_recv()
        for flow in range(7):
            arrival(flow, t, "me").wait_send()
        return 0
    lax.fori_loop(0, n_tile, finish, 0)

    def norm(i, _):
        for q in range(4):
            rows = pl.ds(pl.multiple_of(i * 16, 16), 16)
            v = rall[q, rows, :].astype(F32)
            ms = jnp.mean(v * v, axis=1, keepdims=True)
            u_ref[q, rows, :] = (v * lax.rsqrt(ms + EPSILON) * g_ref[...]).astype(BF)
        return 0
    lax.fori_loop(0, 2 * B // 16, norm, 0)
    r_ref[...] = rall[me, mine, :]


def out_proj(o, x, g2, w_out):
    B, D = x.shape
    K = o.shape[1]
    vm = pl.BlockSpec(memory_space=pltpu.VMEM)
    n_tile = D // 2 // RT
    dma = pltpu.SemaphoreType.DMA
    u, r = pl.pallas_call(
        out_kernel,
        in_specs=[vm, vm, vm, pl.BlockSpec(memory_space=pl.ANY)],
        out_specs=[vm, vm],
        out_shape=[jax.ShapeDtypeStruct((4, 2 * B, D), BF), jax.ShapeDtypeStruct((B, D), BF)],
        scratch_shapes=[pltpu.VMEM((2 * B, K), BF), pltpu.VMEM((2 * B, D // 2), BF), pltpu.VMEM((4, 2 * B, D), BF),
                        pltpu.VMEM((2, K, RT), BF), dma((2,)), dma((4,)), dma((7, n_tile)), dma((7, n_tile))],
        compiler_params=pltpu.CompilerParams(vmem_limit_bytes=VMEM_BYTES, collective_id=1, has_side_effects=True),
        cost_estimate=pl.CostEstimate(flops=2 * B * K * D, bytes_accessed=K * D, transcendentals=0),
        name="out_proj",
    )(o, x, g2.reshape(1, D), w_out.reshape(K, D))
    return u.reshape(8 * B, D), r


DT = LATENT


def down_kernel(y_ref, r_ref, w_hbm, out_ref, part, dbuf, ra, rb, wbuf, wsems, ssems, rsems):
    core, chips, partner, xn, yn = here()
    B, D = r_ref.shape
    n_tile = D // DT
    mine = pl.ds(pl.multiple_of(core * B, B), B)
    theirs = pl.ds(pl.multiple_of((1 - core) * B, B), B)

    def load_w(t, slot):
        return pltpu.make_async_copy(w_hbm.at[:, pl.ds(pl.multiple_of(t * DT, DT), DT)], wbuf.at[slot], wsems.at[slot])
    load_w(0, 0).start()
    load_w(1, 1).start()
    greet((partner, xn, yn))

    def swap(t):
        return remote(part.at[t, :, theirs, :], dbuf.at[t], ssems.at[0, t], rsems.at[0, t], partner)

    def first(k, t, par):
        chip = (("xn", "diag"), ("yn", "diag"))[par][k]
        return remote(part.at[t, chips[chip], mine, :], ra.at[t, k], ssems.at[1 + k, t], rsems.at[1 + k, t], (xn, yn)[par])

    def second(t, par):
        return remote(part.at[t, chips[("yn", "xn")[par]], mine, :], rb.at[t], ssems.at[3, t], rsems.at[3, t], (yn, xn)[par])

    def stage_a(t, par):
        swap(t).wait_recv()
        for chip in (("xn", "yn")[par], "diag", ("yn", "xn")[par], "me"):
            q = chips[chip]
            part[t, q, mine, :] = part[t, q, mine, :] + dbuf[t, q]
        for k in (1, 0):
            first(k, t, par).start()

    def pair(i, _):
        for par in range(2):
            t = 2 * i + par
            load_w(t, par).wait()

            def rows(q, _):
                yq = y_ref[pl.ds(pl.multiple_of(q * 2 * B, 2 * B), 2 * B), :]
                part[t, q] = jnp.dot(yq, wbuf[par], preferred_element_type=F32)
                return 0
            lax.fori_loop(0, 4, rows, 0)
            swap(t).start()

            @pl.when(i < n_tile // 2 - 1)
            def _():
                load_w(t + 2, par).start()
            if par == 1:
                stage_a(t - 1, 0)
            else:
                @pl.when(i > 0)
                def _():
                    stage_a(t - 1, 1)
        return 0
    lax.fori_loop(0, n_tile // 2, pair, 0)
    stage_a(n_tile - 1, 1)

    def stage_b(i, _):
        for par in range(2):
            t = 2 * i + par
            first(1, t, par).wait_recv()
            q = chips[("yn", "xn")[par]]
            part[t, q, mine, :] = part[t, q, mine, :] + ra[t, 1]
            second(t, par).start()
        return 0
    lax.fori_loop(0, n_tile // 2, stage_b, 0)

    def stage_c(i, _):
        for par in range(2):
            t = 2 * i + par
            first(0, t, par).wait_recv()
            second(t, par).wait_recv()
            c = pl.ds(pl.multiple_of(t * DT, DT), DT)
            total = part[t, chips["me"], mine, :] + ra[t, 0] + rb[t]
            out_ref[:, c] = (r_ref[:, c].astype(F32) + total).astype(BF)
            swap(t).wait_send()
            first(0, t, par).wait_send()
            first(1, t, par).wait_send()
            second(t, par).wait_send()
        return 0
    lax.fori_loop(0, n_tile // 2, stage_c, 0)


def down(y, r, w_down):
    B, D = r.shape
    K = y.shape[1]
    n_tile = D // DT
    vm = pl.BlockSpec(memory_space=pltpu.VMEM)
    dma = pltpu.SemaphoreType.DMA
    return pl.pallas_call(
        down_kernel,
        in_specs=[vm, vm, pl.BlockSpec(memory_space=pl.ANY)],
        out_specs=vm,
        out_shape=jax.ShapeDtypeStruct((B, D), BF),
        scratch_shapes=[pltpu.VMEM((n_tile, 4, 2 * B, DT), F32), pltpu.VMEM((n_tile, 4, B, DT), F32), pltpu.VMEM((n_tile, 2, B, DT), F32),
                        pltpu.VMEM((n_tile, B, DT), F32), pltpu.VMEM((2, K, DT), BF), dma((2,)), dma((4, n_tile)), dma((4, n_tile))],
        compiler_params=pltpu.CompilerParams(vmem_limit_bytes=VMEM_BYTES, collective_id=2, has_side_effects=True),
        cost_estimate=pl.CostEstimate(flops=2 * 8 * B * K * D, bytes_accessed=2 * K * D, transcendentals=0),
        name="down",
    )(y, r, w_down)


def rms_norm(values_in, gain_vec):
    floats = values_in.astype(jnp.float32)
    mean_sq = jnp.mean(floats * floats, axis=-1, keepdims=True)
    return floats * lax.rsqrt(mean_sq + EPSILON) * gain_vec


def apply_rope(values_in, cos_t, sin_t):
    half_dim = values_in.shape[-1] // 2
    low_half = values_in[..., :half_dim]
    high_half = values_in[..., half_dim:]
    return jnp.concatenate([low_half * cos_t - high_half * sin_t, high_half * cos_t + low_half * sin_t], axis=-1)


def attention_rows(hidden, ckv_cache, kpe_cache, cache_len, rope_cos, rope_sin, norm_attn, w_dq, norm_q, w_uq, w_dkv, norm_kv, w_uk, w_uv):
    value_dim = w_uk.shape[0]
    score_scale = MSCALE * MSCALE / math.sqrt(w_uq.shape[2])
    normed = rms_norm(hidden, norm_attn).astype(BF)
    q_latent = rms_norm(jnp.dot(normed, w_dq, preferred_element_type=jnp.float32), norm_q).astype(BF)
    kv_full = jnp.dot(normed, w_dkv, preferred_element_type=jnp.float32)
    ckv_new = rms_norm(kv_full[:, :value_dim], norm_kv).astype(BF)
    kpe_new = apply_rope(kv_full[:, value_dim:], rope_cos, rope_sin).astype(BF)
    qn, qr = uq(q_latent, w_uq, jnp.concatenate([rope_cos, rope_cos], axis=1), jnp.concatenate([-rope_sin, rope_sin], axis=1))
    ql = uk(qn, w_uk)
    ol = attn(score_scale, cache_len, ql, qr, ckv_cache, kpe_cache, ckv_new, kpe_new)
    head_out = uv(ol, w_uv)
    return head_out, ckv_new, kpe_new


def solution(mesh):
    row_spec = P(('rep', 'dp'), None)
    cube_spec = P(('rep', 'dp'), None, None)
    full_spec = P()
    in_specs = (row_spec, cube_spec, cube_spec, P(('rep', 'dp')), row_spec, row_spec,
                full_spec, full_spec, full_spec, full_spec, full_spec, full_spec, full_spec, full_spec, full_spec, full_spec,
                P(None, 'dp'), P(None, 'dp'), P('dp', None))

    def local_step(hidden, ckv_cache, kpe_cache, cache_len, rope_cos, rope_sin, norm_attn, w_dq, norm_q, w_uq, w_dkv, norm_kv, w_uk, w_uv, w_out, norm_mlp, w_gate, w_up, w_down):
        head_out, ckv_new, kpe_new = attention_rows(hidden, ckv_cache, kpe_cache, cache_len, rope_cos, rope_sin, norm_attn, w_dq, norm_q, w_uq, w_dkv, norm_kv, w_uk, w_uv)
        group_in, residual = out_proj(head_out, hidden, norm_mlp, w_out)
        gate_val = jnp.dot(group_in, w_gate, preferred_element_type=jnp.float32)
        up_val = jnp.dot(group_in, w_up, preferred_element_type=jnp.float32)
        act_val = (jax.nn.silu(gate_val) * up_val).astype(BF)
        out_hidden = down(act_val, residual, w_down)
        return out_hidden, ckv_new, kpe_new

    return jax.shard_map(local_step, mesh=mesh, in_specs=in_specs, out_specs=(row_spec, row_spec, row_spec), check_vma=False)
```

```python
import functools
import math
import jax
import jax.numpy as jnp
from jax import lax
from jax.experimental import pallas as pl
from jax.experimental.pallas import tpu as pltpu
from jax.sharding import PartitionSpec as P

EPSILON = 1e-6
MSCALE = 0.1 * math.log(40.0) + 1.0
BF = jnp.bfloat16
F32 = jnp.float32
LANES = 128
WIDE = 256
LATENT = 512
NT = (((1,), (1,)), ((), ()))
VMEM_BYTES = 60 * 1024 * 1024
QS = 200
HS = 72
LC = 256


def loop(count, body, unroll=1):
    lax.fori_loop(0, count, body, 0, unroll=unroll)


def start_rows(w_hbm, buf, sem, l0, count):
    def one(l, _):
        pltpu.make_async_copy(w_hbm.at[l0 + l], buf.at[:, pl.ds(pl.multiple_of(2 * l, 2), 2), :], sem).start()
        return 0
    loop(count, one, unroll=8)


def spread(par):
    rows = lax.broadcasted_iota(jnp.int32, (LANES, WIDE), 0)
    cols = lax.broadcasted_iota(jnp.int32, (LANES, WIDE), 1)
    return jnp.where(cols == 2 * rows + par, 1.0, 0.0).astype(BF)


def uq_kernel(cq_ref, cos_ref, sin_ref, w_hbm, qn_ref, qr_ref, buf, acc, a2, q_scr, h_scr, sems):
    n_chunk = w_hbm.shape[0] // LC
    B = cq_ref.shape[0]
    P = w_hbm.shape[1]
    start_rows(w_hbm, buf.at[0], sems.at[0], 0, LC)
    for par in range(2):
        x = spread(par)
        for k in range(cq_ref.shape[1] // LANES):
            a2[par * B:(par + 1) * B, k * WIDE:(k + 1) * WIDE] = jnp.dot(
                cq_ref[:, k * LANES:(k + 1) * LANES], x, preferred_element_type=F32).astype(BF)
    for c in range(n_chunk):
        slot = c % 2
        if c + 1 < n_chunk:
            start_rows(w_hbm, buf.at[1 - slot], sems.at[1 - slot], (c + 1) * LC, LC)
        pltpu.make_async_copy(buf.at[slot], buf.at[slot], sems.at[slot]).wait()
        lhs = a2[:, c * 2 * LC:(c + 1) * 2 * LC]

        def body(j, _):
            rhs = jnp.concatenate([buf[slot, 2 * j], buf[slot, 2 * j + 1]], axis=1)
            out = jnp.dot(lhs, rhs, preferred_element_type=F32)
            r0 = pl.multiple_of(j * 2 * B, 2 * B)
            if c > 0:
                out = out + acc[pl.ds(r0, 2 * B), :]
            if c < n_chunk - 1:
                acc[pl.ds(r0, 2 * B), :] = out
            else:
                for half in range(2):
                    for par in range(2):
                        q_scr[pl.ds(4 * j + 2 * half + par, B, stride=QS), :] = out[par * B:(par + 1) * B, half * LANES:(half + 1) * LANES]
            return 0
        loop(P // 2, body, unroll=8)

    def tb(b, _):
        blk = q_scr[pl.ds(pl.multiple_of(b * QS, 8), 192), :]
        h_scr[pl.ds(b, LANES, stride=HS), :] = blk[:LANES].T
        v = blk[LANES:192].T
        rot = jnp.concatenate([v[:, 32:], v[:, :32]], axis=1)
        qr_ref[b] = (v * cos_ref[pl.ds(b, 1), :] + rot * sin_ref[pl.ds(b, 1), :]).astype(BF)
        return 0
    loop(B, tb, unroll=8)

    def hb(h, _):
        qn_ref[h] = h_scr[pl.ds(pl.multiple_of(h * HS, 8), B), :].astype(BF)
        return 0
    loop(LANES, hb, unroll=8)


def uq(cq, w_uq, cos2, sin2):
    B, L = cq.shape
    w4 = w_uq.transpose(0, 2, 1).reshape(L, 96, 2, LANES)
    vm = pl.BlockSpec(memory_space=pltpu.VMEM)
    return pl.pallas_call(
        uq_kernel,
        in_specs=[vm, vm, vm, pl.BlockSpec(memory_space=pl.ANY)],
        out_specs=[vm, vm],
        out_shape=[jax.ShapeDtypeStruct((LANES, B, LANES), BF), jax.ShapeDtypeStruct((B, LANES, 64), BF)],
        scratch_shapes=[pltpu.VMEM((2, 96, 2 * LC, LANES), BF), pltpu.VMEM((96 * B, WIDE), F32), pltpu.VMEM((2 * B, 2 * L), BF),
                        pltpu.VMEM((B * QS, LANES), F32), pltpu.VMEM((LANES * HS, LANES), F32), pltpu.SemaphoreType.DMA((2,))],
        compiler_params=pltpu.CompilerParams(vmem_limit_bytes=VMEM_BYTES),
        cost_estimate=pl.CostEstimate(flops=2 * B * L * 24576, bytes_accessed=76 * 10**6, transcendentals=0),
        name="uq",
    )(cq, cos2, sin2, w4)


UL = LANES
KS = 136


def uk_kernel(qn_ref, w_hbm, ql_ref, buf, scr, wd, sel, sems):
    B = qn_ref.shape[1]
    n_chunk = w_hbm.shape[0] // UL
    P = w_hbm.shape[1]
    start_rows(w_hbm, buf.at[0], sems.at[0], 0, UL)
    sel[0:LANES] = spread(0)
    sel[LANES:WIDE] = spread(1)
    for c in range(n_chunk):
        slot = c % 2
        if c + 1 < n_chunk:
            start_rows(w_hbm, buf.at[1 - slot], sems.at[1 - slot], (c + 1) * UL, UL)
        pltpu.make_async_copy(buf.at[slot], buf.at[slot], sems.at[slot]).wait()

        def sort(j, _):
            rhs = jnp.concatenate([buf[slot, 2 * j], buf[slot, 2 * j + 1]], axis=1)
            wd[j] = jnp.dot(sel[...], rhs, preferred_element_type=F32).astype(BF)
            return 0
        loop(P // 2, sort, unroll=8)

        def body(j, _):
            for half in range(2):
                for par in range(2):
                    h = 4 * j + 2 * half + par
                    scr[pl.ds(h, B, stride=KS), :] = lax.dot_general(
                        qn_ref[h], wd[j, par * UL:(par + 1) * UL, half * LANES:(half + 1) * LANES],
                        NT, preferred_element_type=F32)
            return 0
        loop(P // 2, body, unroll=4)

        def cb(b, _):
            ql_ref[b, :, c * UL:(c + 1) * UL] = scr[pl.ds(pl.multiple_of(b * KS, 8), LANES), :].astype(BF)
            return 0
        loop(B, cb, unroll=4)


def uk(qn, w_uk):
    B = qn.shape[1]
    vm = pl.BlockSpec(memory_space=pltpu.VMEM)
    return pl.pallas_call(
        uk_kernel,
        in_specs=[vm, pl.BlockSpec(memory_space=pl.ANY)],
        out_specs=vm,
        out_shape=jax.ShapeDtypeStruct((B, LANES, LATENT), BF),
        scratch_shapes=[pltpu.VMEM((2, 64, 2 * UL, LANES), BF), pltpu.VMEM((B * KS, LANES), F32), pltpu.VMEM((32, WIDE, WIDE), BF), pltpu.VMEM((WIDE, WIDE), BF),
                        pltpu.SemaphoreType.DMA((2,))],
        compiler_params=pltpu.CompilerParams(vmem_limit_bytes=VMEM_BYTES),
        cost_estimate=pl.CostEstimate(flops=2 * B * LANES * LANES * LATENT, bytes_accessed=26 * 10**6, transcendentals=0),
        name="uk",
    )(qn, w_uk.reshape(LATENT, 64, 2, LANES))


NB = 4


def attn_kernel(scale, len_ref, ql_ref, qr_ref, ckv_ref, kpe_ref, cn_ref, kn_ref, ol_ref):
    T = ckv_ref.shape[1]
    dn = NT
    for i in range(NB):
        pos = len_ref[pl.program_id(0) * NB + i]
        row = lax.broadcasted_iota(jnp.int32, ckv_ref.shape[1:], 0)
        ckv = jnp.where(row == pos, cn_ref[i], ckv_ref[i])
        lane = lax.broadcasted_iota(jnp.int32, (LANES, T), 1)
        kn = jnp.broadcast_to(kn_ref[i], (T, 64))
        s_new = lax.dot_general(qr_ref[i], kn, dn, preferred_element_type=F32)
        s_pe = jnp.dot(qr_ref[i], kpe_ref[i], preferred_element_type=F32)
        s = lax.dot_general(ql_ref[i], ckv, dn, preferred_element_type=F32)
        s = (s + jnp.where(lane == pos, s_new, s_pe)) * scale
        s = jnp.where(lane <= pos, s, -jnp.inf)
        e = jnp.exp(s - jnp.max(s, axis=1, keepdims=True))
        den = jnp.sum(e, axis=1, keepdims=True)
        ol = jnp.dot(e.astype(BF), ckv, preferred_element_type=F32)
        ol = (ol / den).astype(BF)
        for k in range(4):
            ol_ref[i, k] = ol[:, k * LANES:(k + 1) * LANES]


def attn(scale, length, ql, qr, ckv, kpe, c_new, k_new):
    B, T, L = ckv.shape
    spec = lambda *s: pl.BlockSpec((NB,) + s, lambda i, _: (i, 0, 0))
    return pl.pallas_call(
        functools.partial(attn_kernel, scale),
        grid_spec=pltpu.PrefetchScalarGridSpec(
            num_scalar_prefetch=1, grid=(B // NB,),
            in_specs=[spec(LANES, L), spec(LANES, 64), spec(T, L), spec(64, T), spec(1, L), spec(1, 64)],
            out_specs=pl.BlockSpec((NB, 4, LANES, LANES), lambda i, _: (i, 0, 0, 0))),
        out_shape=jax.ShapeDtypeStruct((B, 4, LANES, LANES), BF),
        compiler_params=pltpu.CompilerParams(vmem_limit_bytes=40 * 2**20),
        cost_estimate=pl.CostEstimate(flops=2 * B * LANES * T * 1100, bytes_accessed=40 * 10**6, transcendentals=B * LANES * T),
        name="attn",
    )(length, ql, qr, ckv, kpe.transpose(0, 2, 1), c_new.reshape(B, 1, L), k_new.reshape(B, 1, 64))


VP = 16


def uv_kernel(ol_hbm, w_hbm, o_ref, wbuf, abuf, wd, mid, sel, wsems, asem):
    B = ol_hbm.shape[0]
    n_chunk = 64 // VP

    def start_w(c, slot):
        def one(l, _):
            pltpu.make_async_copy(w_hbm.at[l, pl.ds(c * VP, VP)], wbuf.at[slot, :, pl.ds(pl.multiple_of(2 * l, 2), 2), :], wsems.at[slot]).start()
            return 0
        loop(LATENT, one, unroll=8)
    def start_a(b, _):
        pltpu.make_async_copy(ol_hbm.at[b], abuf.at[:, :, pl.ds(pl.multiple_of(2 * b, 2), 2), :], asem).start()
        return 0
    loop(B, start_a, unroll=8)
    start_w(0, 0)
    sel[0:LANES] = spread(0)
    sel[LANES:WIDE] = spread(1)
    half_rows = lax.broadcasted_iota(jnp.int32, (2 * B, 2 * B), 0)
    half_cols = lax.broadcasted_iota(jnp.int32, (2 * B, 2 * B), 1)
    want = jnp.where(half_rows < B, 2 * half_rows, 2 * (half_rows - B) + 1)
    pick = jnp.where(half_cols == want, 1.0, 0.0).astype(BF)
    pltpu.make_async_copy(abuf, abuf, asem).wait()
    for c in range(n_chunk):
        slot = c % 2
        if c + 1 < n_chunk:
            start_w(c + 1, 1 - slot)
        pltpu.make_async_copy(wbuf.at[slot], wbuf.at[slot], wsems.at[slot]).wait()

        def sort(j, _):
            for k in range(4):
                rows = slice(k * WIDE, (k + 1) * WIDE)
                rhs = jnp.concatenate([wbuf[slot, 2 * j, rows], wbuf[slot, 2 * j + 1, rows]], axis=1)
                w = jnp.dot(sel[...], rhs, preferred_element_type=F32).astype(BF)
                for half in range(2):
                    for par in range(2):
                        wd[2 * j + half, k * LANES:(k + 1) * LANES, par * LANES:(par + 1) * LANES] = w[par * LANES:(par + 1) * LANES, half * LANES:(half + 1) * LANES]
            return 0
        loop(VP // 2, sort, unroll=2)

        def body(j, _):
            p = c * VP + j
            lhs = jnp.concatenate([abuf[k, p] for k in range(4)], axis=1)
            mid[j] = jnp.dot(lhs, wd[j], preferred_element_type=F32).astype(BF)
            return 0
        loop(VP, body, unroll=4)

        def put(j, _):
            r = jnp.dot(pick, mid[j], preferred_element_type=F32).astype(BF)
            col = pl.multiple_of((c * VP + j) * WIDE, WIDE)
            o_ref[:, pl.ds(col, LANES)] = r[0:B, 0:LANES]
            o_ref[:, pl.ds(col + LANES, LANES)] = r[B:2 * B, LANES:WIDE]
            return 0
        loop(VP, put, unroll=4)


def uv(ol, w_uv):
    B = ol.shape[0]
    return pl.pallas_call(
        uv_kernel,
        in_specs=[pl.BlockSpec(memory_space=pl.ANY)] * 2,
        out_specs=pl.BlockSpec(memory_space=pltpu.VMEM),
        out_shape=jax.ShapeDtypeStruct((B, LANES * LANES), BF),
        scratch_shapes=[pltpu.VMEM((2, VP, 1024, LANES), BF), pltpu.VMEM((4, 64, 2 * B, LANES), BF), pltpu.VMEM((VP, LATENT, WIDE), BF), pltpu.VMEM((VP, 2 * B, WIDE), BF), pltpu.VMEM((WIDE, WIDE), BF),
                        pltpu.SemaphoreType.DMA((2,)), pltpu.SemaphoreType.DMA],
        compiler_params=pltpu.CompilerParams(vmem_limit_bytes=VMEM_BYTES),
        cost_estimate=pl.CostEstimate(flops=2 * B * LANES * LANES * LATENT, bytes_accessed=26 * 10**6, transcendentals=0),
        name="uv",
    )(ol.reshape(B, 4, 64, 2, LANES), w_uv.reshape(LATENT, 64, 2, LANES))

def here():
    d = lax.axis_index("dp")
    core = lax.rem(d, 2)
    x = lax.rem(d // 2, 2)
    y = d // 4
    partner = {"dp": d + 1 - 2 * core}
    xn = {"dp": d + 2 - 4 * x}
    yn = {"dp": d + 4 - 8 * y}
    chips = dict(me=2 * y + x, xn=2 * y + 1 - x, yn=2 * (1 - y) + x, diag=2 * (1 - y) + 1 - x)
    return core, chips, partner, xn, yn


def greet(devices):
    barrier = pltpu.get_barrier_semaphore()
    for dev in devices:
        pl.semaphore_signal(barrier, inc=1, device_id=dev, device_id_type=pl.DeviceIdType.MESH)
    pl.semaphore_wait(barrier, len(devices))


def remote(src, dst, send_sem, recv_sem, dev):
    return pltpu.make_async_remote_copy(src_ref=src, dst_ref=dst, send_sem=send_sem, recv_sem=recv_sem,
                                        device_id=dev, device_id_type=pl.DeviceIdType.MESH)


RT = WIDE


def out_kernel(o_ref, x_ref, g_ref, w_hbm, u_ref, r_ref, o2, x2, rall, wbuf, wsems, osems, ssems, rsems):
    core, chips, partner, xn, yn = here()
    me = chips["me"]
    D = x_ref.shape[1]
    half = D // 2
    K = o_ref.shape[1]
    B = o_ref.shape[0]
    n_tile = half // RT
    mine = pl.ds(pl.multiple_of(core * B, B), B)

    def cols(t):
        return pl.ds(pl.multiple_of(core * half + t * RT, RT), RT)

    def load_w(t, slot):
        return pltpu.make_async_copy(w_hbm.at[:, cols(t)], wbuf.at[slot], wsems.at[slot])
    load_w(0, 0).start()
    load_w(1, 1).start()
    greet((partner, xn, yn))
    send_o = remote(o_ref, o2.at[mine], osems.at[0], osems.at[1], partner)
    send_o.start()
    theirs = pl.ds(pl.multiple_of((1 - core) * half, half), half)
    send_x = remote(x_ref.at[:, theirs], x2.at[mine], osems.at[2], osems.at[3], partner)
    send_x.start()
    o2[mine, :] = o_ref[...]
    x2[mine, :] = x_ref[:, pl.ds(pl.multiple_of(core * half, half), half)]

    def copy(flow, t, chip, dev):
        ref = rall.at[chips[chip], :, cols(t)]
        return remote(ref, ref, ssems.at[flow, t], rsems.at[flow, t], dev)

    def arrival(flow, t, chip):
        ref = rall.at[chips[chip], :, cols(t)]
        return remote(ref, ref, ssems.at[flow, t], rsems.at[flow, t], partner)

    def first_forwards(t, par):
        arrival(1, t, "xn").wait_recv()
        copy(3, t, "xn", partner).start()
        if par == 0:
            copy(4, t, "xn", yn).start()
        arrival(2, t, "yn").wait_recv()
        copy(5, t, "yn", partner).start()
        if par == 1:
            copy(4, t, "yn", xn).start()

    def last_forward(t):
        arrival(4, t, "diag").wait_recv()
        copy(6, t, "diag", partner).start()
    send_o.wait()
    send_x.wait()

    def pair(i, _):
        for par in range(2):
            t = 2 * i + par
            load_w(t, par).wait()
            def dot_k(k, acc):
                rows = pl.ds(pl.multiple_of(k * 2048, 2048), 2048)
                return acc + jnp.dot(o2[:, rows], wbuf[par, rows, :], preferred_element_type=F32)
            acc = lax.fori_loop(0, K // 2048, dot_k, jnp.zeros((2 * B, RT), F32), unroll=4)
            xt = x2[:, pl.ds(pl.multiple_of(t * RT, RT), RT)].astype(F32)
            rall[me, :, cols(t)] = (xt + acc).astype(BF)

            @pl.when(i < n_tile // 2 - 1)
            def _():
                load_w(t + 2, par).start()
            copy(0, t, "me", partner).start()
            copy(1, t, "me", xn).start()
            copy(2, t, "me", yn).start()

            @pl.when(i > 0)
            def _():
                first_forwards(t - 2, par)

            @pl.when(i > 1)
            def _():
                last_forward(t - 4)
        return 0
    loop(n_tile // 2, pair)
    for par in range(2):
        first_forwards(n_tile - 2 + par, par)
    for t in range(n_tile - 4, n_tile):
        last_forward(t)

    def finish(t, _):
        other = pl.ds(pl.multiple_of((1 - core) * half + t * RT, RT), RT)
        for flow, chip in ((0, "me"), (3, "xn"), (5, "yn"), (6, "diag")):
            ref = rall.at[chips[chip], :, other]
            remote(ref, ref, ssems.at[flow, t], rsems.at[flow, t], partner).wait_recv()
        for flow in range(7):
            arrival(flow, t, "me").wait_send()
        return 0
    loop(n_tile, finish)

    def norm(i, _):
        for k, chip in enumerate(("me", "xn", "yn", "diag")):
            rows = pl.ds(pl.multiple_of(i * 16, 16), 16)
            v = rall[chips[chip], rows, :].astype(F32)
            ms = jnp.mean(v * v, axis=1, keepdims=True)
            u_ref[k, rows, :] = (v * lax.rsqrt(ms + EPSILON) * g_ref[...]).astype(BF)
        return 0
    loop(2 * B // 16, norm)
    r_ref[...] = rall[me, mine, :]


def out_proj(o, x, g2, w_out):
    B, D = x.shape
    K = o.shape[1]
    vm = pl.BlockSpec(memory_space=pltpu.VMEM)
    n_tile = D // 2 // RT
    dma = pltpu.SemaphoreType.DMA
    u, r = pl.pallas_call(
        out_kernel,
        in_specs=[vm, vm, vm, pl.BlockSpec(memory_space=pl.ANY)],
        out_specs=[vm, vm],
        out_shape=[jax.ShapeDtypeStruct((4, 2 * B, D), BF), jax.ShapeDtypeStruct((B, D), BF)],
        scratch_shapes=[pltpu.VMEM((2 * B, K), BF), pltpu.VMEM((2 * B, D // 2), BF), pltpu.VMEM((4, 2 * B, D), BF),
                        pltpu.VMEM((2, K, RT), BF), dma((2,)), dma((4,)), dma((7, n_tile)), dma((7, n_tile))],
        compiler_params=pltpu.CompilerParams(vmem_limit_bytes=VMEM_BYTES, collective_id=1, has_side_effects=True),
        cost_estimate=pl.CostEstimate(flops=2 * B * K * D, bytes_accessed=K * D, transcendentals=0),
        name="out_proj",
    )(o, x, g2.reshape(1, D), w_out.reshape(K, D))
    return u.reshape(8 * B, D), r


DT = LATENT
GT = LANES


def mlp_kernel(u_ref, r_ref, wg_hbm, wu_hbm, w_hbm, out_ref, y, part, dbuf, ra, rb, gbuf, ubuf, wbuf, gsems, usems, wsems, ssems, rsems):
    core, chips, partner, xn, yn = here()
    B, D = r_ref.shape
    n_gate, n_tile = wg_hbm.shape[1] // GT, D // DT
    near, side, far = (1, 2), (2, 1), 3
    others, own = slice(2 * B, 8 * B), slice(0, 2 * B)

    def load_g(n, slot):
        c = pl.ds(pl.multiple_of(n * GT, GT), GT)
        return (pltpu.make_async_copy(wg_hbm.at[:, c], gbuf.at[slot], gsems.at[slot]),
                pltpu.make_async_copy(wu_hbm.at[:, c], ubuf.at[slot], usems.at[slot]))

    def load_w(t, slot):
        return pltpu.make_async_copy(w_hbm.at[:, pl.ds(pl.multiple_of(t * DT, DT), DT)], wbuf.at[slot], wsems.at[slot])

    for slot in range(2):
        for cp in load_g(slot, slot):
            cp.start()
    for slot in range(2):
        load_w(slot, slot).start()
    greet((partner, xn, yn))

    def gate_up(which, more):
        def step(n, _):
            slot = lax.rem(n, 2)
            for cp in load_g(n, slot):
                cp.wait()

            uq = u_ref[which, :]
            both = jnp.dot(uq, jnp.concatenate([gbuf[slot], ubuf[slot]], axis=1), preferred_element_type=F32)
            y[which, pl.ds(pl.multiple_of(n * GT, GT), GT)] = (jax.nn.silu(both[:, :GT]) * both[:, GT:]).astype(BF)

            @pl.when(n < n_gate - 2)
            def _():
                for cp in load_g(n + 2, slot):
                    cp.start()
            if more:
                @pl.when(n >= n_gate - 2)
                def _():
                    for cp in load_g(slot, slot):
                        cp.start()
            return 0
        loop(n_gate, step)

    def mine(k):
        return pl.ds(pl.multiple_of((2 * k + core) * B, B), B)

    def theirs(k):
        return pl.ds(pl.multiple_of((2 * k + 1 - core) * B, B), B)

    def swap(k, t):
        return remote(part.at[t, theirs(k), :], dbuf.at[t, k], ssems.at[3 + k, t], rsems.at[3 + k, t], partner)

    def first(k, t, par):
        return remote(part.at[t, mine((near[par], far)[k]), :], ra.at[t, k], ssems.at[k, t], rsems.at[k, t], (xn, yn)[par])

    def second(t, par):
        return remote(part.at[t, mine(side[par]), :], rb.at[t], ssems.at[2, t], rsems.at[2, t], (yn, xn)[par])

    def stage_a(t, par):
        for k in (far, near[par], side[par]):
            swap(k, t).wait_recv()
            part[t, mine(k), :] = part[t, mine(k), :] + dbuf[t, k]
        for k in (1, 0):
            first(k, t, par).start()

    def down(which, send, more, after):
        def pair(i, _):
            for par in range(2):
                t = 2 * i + par
                load_w(t, par).wait()

                part[t, which, :] = jnp.dot(y[which, :], wbuf[par], preferred_element_type=F32)
                for k in send:
                    swap(k, t).start()

                @pl.when(i < n_tile // 2 - 1)
                def _():
                    load_w(t + 2, par).start()
                if more:
                    @pl.when(i == n_tile // 2 - 1)
                    def _():
                        load_w(par, par).start()
                if after and par == 1:
                    after(t - 1, 0)
                elif after:
                    @pl.when(i > 0)
                    def _():
                        after(t - 1, 1)
            return 0
        loop(n_tile // 2, pair)

    gate_up(others, True)
    down(others, (3, 1, 2), True, stage_a)
    stage_a(n_tile - 1, 1)
    gate_up(own, False)
    down(own, (0,), False, None)

    def stage_b(i, _):
        for par in range(2):
            t = 2 * i + par
            first(1, t, par).wait_recv()
            part[t, mine(side[par]), :] = part[t, mine(side[par]), :] + ra[t, 1]
            second(t, par).start()
        return 0
    loop(n_tile // 2, stage_b)

    def stage_c(i, _):
        for par in range(2):
            t = 2 * i + par
            swap(0, t).wait_recv()
            first(0, t, par).wait_recv()
            second(t, par).wait_recv()
            c = pl.ds(pl.multiple_of(t * DT, DT), DT)
            total = part[t, mine(0), :] + dbuf[t, 0] + ra[t, 0] + rb[t]
            out_ref[:, c] = (r_ref[:, c].astype(F32) + total).astype(BF)
            for cp in (swap(0, t), swap(1, t), swap(2, t), swap(3, t), first(0, t, par), first(1, t, par), second(t, par)):
                cp.wait_send()
        return 0
    loop(n_tile // 2, stage_c)


def mlp(u, r, w_gate, w_up, w_down):
    B, D = r.shape
    K = w_down.shape[0]
    n_tile = D // DT
    vm = pl.BlockSpec(memory_space=pltpu.VMEM)
    dma = pltpu.SemaphoreType.DMA
    return pl.pallas_call(
        mlp_kernel,
        in_specs=[vm, vm] + [pl.BlockSpec(memory_space=pl.ANY)] * 3,
        out_specs=vm,
        out_shape=jax.ShapeDtypeStruct((B, D), BF),
        scratch_shapes=[pltpu.VMEM((8 * B, K), BF), pltpu.VMEM((n_tile, 8 * B, DT), F32), pltpu.VMEM((n_tile, 4, B, DT), F32),
                        pltpu.VMEM((n_tile, 2, B, DT), F32), pltpu.VMEM((n_tile, B, DT), F32), pltpu.VMEM((2, D, GT), BF),
                        pltpu.VMEM((2, D, GT), BF), pltpu.VMEM((2, K, DT), BF), dma((2,)), dma((2,)), dma((2,)), dma((7, n_tile)), dma((7, n_tile))],
        compiler_params=pltpu.CompilerParams(vmem_limit_bytes=VMEM_BYTES, collective_id=2, has_side_effects=True),
        cost_estimate=pl.CostEstimate(flops=48 * B * K * D, bytes_accessed=6 * K * D, transcendentals=0),
        name="mlp",
    )(u, r, w_gate, w_up, w_down)


def rms_norm(values_in, gain_vec):
    floats = values_in.astype(jnp.float32)
    mean_sq = jnp.mean(floats * floats, axis=-1, keepdims=True)
    return floats * lax.rsqrt(mean_sq + EPSILON) * gain_vec


def apply_rope(values_in, cos_t, sin_t):
    half_dim = values_in.shape[-1] // 2
    low_half = values_in[..., :half_dim]
    high_half = values_in[..., half_dim:]
    return jnp.concatenate([low_half * cos_t - high_half * sin_t, high_half * cos_t + low_half * sin_t], axis=-1)


def attention_rows(hidden, ckv_cache, kpe_cache, cache_len, rope_cos, rope_sin, norm_attn, w_dq, norm_q, w_uq, w_dkv, norm_kv, w_uk, w_uv):
    value_dim = w_uk.shape[0]
    score_scale = MSCALE * MSCALE / math.sqrt(w_uq.shape[2])
    normed = rms_norm(hidden, norm_attn).astype(BF)
    q_latent = rms_norm(jnp.dot(normed, w_dq, preferred_element_type=jnp.float32), norm_q).astype(BF)
    kv_full = jnp.dot(normed, w_dkv, preferred_element_type=jnp.float32)
    ckv_new = rms_norm(kv_full[:, :value_dim], norm_kv).astype(BF)
    kpe_new = apply_rope(kv_full[:, value_dim:], rope_cos, rope_sin).astype(BF)
    qn, qr = uq(q_latent, w_uq, jnp.concatenate([rope_cos, rope_cos], axis=1), jnp.concatenate([-rope_sin, rope_sin], axis=1))
    ql = uk(qn, w_uk)
    ol = attn(score_scale, cache_len, ql, qr, ckv_cache, kpe_cache, ckv_new, kpe_new)
    head_out = uv(ol, w_uv)
    return head_out, ckv_new, kpe_new


def solution(mesh):
    row_spec = P(('rep', 'dp'), None)
    cube_spec = P(('rep', 'dp'), None, None)
    full_spec = P()
    in_specs = (row_spec, cube_spec, cube_spec, P(('rep', 'dp')), row_spec, row_spec,
                full_spec, full_spec, full_spec, full_spec, full_spec, full_spec, full_spec, full_spec, full_spec, full_spec,
                P(None, 'dp'), P(None, 'dp'), P('dp', None))

    def local_step(hidden, ckv_cache, kpe_cache, cache_len, rope_cos, rope_sin, norm_attn, w_dq, norm_q, w_uq, w_dkv, norm_kv, w_uk, w_uv, w_out, norm_mlp, w_gate, w_up, w_down):
        head_out, ckv_new, kpe_new = attention_rows(hidden, ckv_cache, kpe_cache, cache_len, rope_cos, rope_sin, norm_attn, w_dq, norm_q, w_uq, w_dkv, norm_kv, w_uk, w_uv)
        group_in, residual = out_proj(head_out, hidden, norm_mlp, w_out)
        out_hidden = mlp(group_in, residual, w_gate, w_up, w_down)
        return out_hidden, ckv_new, kpe_new

    return jax.shard_map(local_step, mesh=mesh, in_specs=in_specs, out_specs=(row_spec, row_spec, row_spec), check_vma=False)
```
